32 devices in a mesh: seg: 8 (over z, core), tok: 4 (over y, x).
Axes of the slice: x: 2, y: 2, z: 4, core: 2. Of those that a mesh axis runs over, the one named last changes fastest.
Arguments:
- queries: bfloat16 [2, 8, 2, 5120, 256], P(None, 'seg', None, 'tok'), may hold values from -6 to 6
- key_vectors: bfloat16 [2, 8, 2, 5120, 256], P(None, 'seg', None, 'tok'), may hold values from -6 to 6
- values: bfloat16 [2, 8, 2, 5120, 256], P(None, 'seg', None, 'tok'), may hold values from -6 to 6
- token_rates: float32 [2, 8, 2, 5120], P(None, 'seg', None, 'tok'), may hold values from 0.05 to 3
- fast_weights: float32 [8, 3, 256, 256], P('seg', None, None, 'tok'), may hold values from -0.375 to 0.375
- momenta: float32 [8, 3, 256, 256], P('seg', None, None, 'tok'), may hold values from -3 to 3
- fresh_weights: float32 [3, 256, 256], P(None, None, 'tok'), may hold values from -0.375 to 0.375
- fresh_momenta: float32 [3, 256, 256], P(None, None, 'tok'), may hold values from -3 to 3
Outputs:
- outputs: bfloat16 [2, 8, 2, 5120, 256], P(None, 'seg', None, 'tok')
- final_weights: float32 [8, 3, 256, 256], P('seg', None, None, 'tok')
- final_momenta: float32 [8, 3, 256, 256], P('seg', None, None, 'tok')
The draws below stay inside these ranges and needn't reach their ends.
All inputs are finite; a program needn't handle non-finite values.
Results may differ from the reference program's by a relative error of at most 0.033.
Values may be sent and summed in bfloat16 or wider, within the bound.
A program may use at most 64 MiB of HBM per device.

```python
import math
import jax
import jax.numpy as jnp
from jax import lax

HEAD = 256
GROUPS = 2
STEPS = 2
SEGS = 8
GROUP = 5120


def draw_token_rates(key, part):
    shape = (STEPS, SEGS, GROUPS, GROUP)
    level = jnp.exp(jax.random.uniform(key, shape, jnp.float32, math.log(0.05), 0.0))
    ramp = 1.0 + 2.0 * jnp.arange(GROUP, dtype=jnp.float32) / GROUP
    return level * ramp


def block_levels(stream_key, extent, shards, least, top_value):
    level = 1.0
    for dim, blocks in shards:
        draws = jax.random.uniform(jax.random.fold_in(jax.random.fold_in(stream_key, 6), dim), (blocks,), jnp.float32, least / len(shards), top_value / len(shards))
        level = level * jnp.repeat(jnp.exp(draws), extent[dim] // blocks).reshape((-1,) + (1,) * (len(extent) - 1 - dim))
    return level


def normal_values(key, shape, scale, reach, pieces=(), kind=jnp.bfloat16):
    values = jax.random.normal(key, shape, jnp.float32) * scale
    if len(pieces) > 0:
        values = block_levels(key, shape, pieces, -0.22, 0.18) * values
    return jnp.clip(values, min=-reach, max=reach).astype(kind)


def setup_inputs(seed: int = 0) -> dict:
    arg_keys = jax.random.split(jax.random.key(seed), 9)
    queries = normal_values(arg_keys[0], (STEPS, SEGS, GROUPS, GROUP, HEAD), 1.0, 6.0, ((1, 8), (3, 4)))
    key_vectors = normal_values(arg_keys[1], (STEPS, SEGS, GROUPS, GROUP, HEAD), 1.0, 6.0, ((1, 8), (3, 4)))
    values = normal_values(arg_keys[2], (STEPS, SEGS, GROUPS, GROUP, HEAD), 1.0, 6.0, ((1, 8), (3, 4)))
    token_rates = draw_token_rates(jax.random.fold_in(arg_keys[8], 71), 0)
    fast_weights = normal_values(arg_keys[4], (SEGS, 3, HEAD, HEAD), HEAD ** -0.5, 0.375, ((0, 8), (3, 4)), jnp.float32)
    momenta = normal_values(arg_keys[5], (SEGS, 3, HEAD, HEAD), 0.5, 3.0, ((0, 8), (3, 4)), jnp.float32)
    fresh_weights = normal_values(arg_keys[6], (3, HEAD, HEAD), HEAD ** -0.5, 0.375, ((2, 4),), jnp.float32)
    fresh_momenta = normal_values(arg_keys[7], (3, HEAD, HEAD), 0.5, 3.0, ((2, 4),), jnp.float32)
    return {"queries": queries, "key_vectors": key_vectors, "values": values, "token_rates": token_rates, "fast_weights": fast_weights, "momenta": momenta, "fresh_weights": fresh_weights, "fresh_momenta": fresh_momenta}


momentum_decay = 0.9
learn_rate = 0.05
epsilon = 1e-06

def silu_parts(pre_gate):
    sigmoid_gate = jax.nn.sigmoid(pre_gate)
    return (pre_gate * sigmoid_gate, sigmoid_gate * (1.0 + pre_gate * (1.0 - sigmoid_gate)))

def local_grads(usable_weights, key_rows, value_rows, rate_rows):
    pre_gate = jnp.dot(key_rows, usable_weights[0], preferred_element_type=jnp.float32)
    pre_up = jnp.dot(key_rows, usable_weights[2], preferred_element_type=jnp.float32)
    active, slope_gate = silu_parts(pre_gate)
    hidden = (active * pre_up).astype(jnp.bfloat16)
    scaled = (rate_rows[:, None] * value_rows.astype(jnp.float32)).astype(jnp.bfloat16)
    back_hidden = -lax.dot_general(scaled, usable_weights[1], (((1,), (1,)), ((), ())), preferred_element_type=jnp.float32)
    back_gate = (back_hidden * pre_up * slope_gate).astype(jnp.bfloat16)
    back_up = (back_hidden * active).astype(jnp.bfloat16)
    contract_rows = (((0,), (0,)), ((), ()))
    grad_gate = lax.dot_general(key_rows, back_gate, contract_rows, preferred_element_type=jnp.float32)
    grad_down = -lax.dot_general(hidden, scaled, contract_rows, preferred_element_type=jnp.float32)
    grad_up = lax.dot_general(key_rows, back_up, contract_rows, preferred_element_type=jnp.float32)
    return (jnp.stack([grad_gate, grad_down, grad_up]), jnp.sum(rate_rows * rate_rows))

def update(weights, moment, gradients, rate_total):
    moment = momentum_decay * moment + gradients * lax.rsqrt(rate_total)
    stepped = weights - learn_rate * moment
    rescale = jnp.sqrt(lax.optimization_barrier(jnp.sum(weights * weights, axis=1, keepdims=True)) / (lax.optimization_barrier(jnp.sum(stepped * stepped, axis=1, keepdims=True)) + epsilon))
    return (stepped * rescale, moment)

def apply_fast(usable_weights, query_rows):
    pre_gate = jnp.dot(query_rows, usable_weights[0], preferred_element_type=jnp.float32)
    pre_up = jnp.dot(query_rows, usable_weights[2], preferred_element_type=jnp.float32)
    hidden = (jax.nn.silu(pre_gate) * pre_up).astype(jnp.bfloat16)
    return jnp.dot(hidden, usable_weights[1], preferred_element_type=jnp.float32).astype(jnp.bfloat16)

def run_segment(inputs):
    weights, moment, query_seg, key_seg, value_seg, rate_seg = inputs
    results = []
    for block_index in range(GROUPS):
        usable_weights = weights.astype(jnp.bfloat16)
        gradients, square = local_grads(usable_weights, key_seg[block_index], value_seg[block_index], rate_seg[block_index])
        weights, moment = update(weights, moment, gradients, square)
        results.append(apply_fast(weights.astype(jnp.bfloat16), query_seg[block_index]))
    return (weights, moment, jnp.stack(results))

def reference(queries, key_vectors, values, token_rates, fast_weights, momenta, fresh_weights, fresh_momenta):
    leave_weights, leave_moment, outputs_first = lax.map(run_segment, (fast_weights, momenta, queries[0], key_vectors[0], values[0], token_rates[0]))
    enter_weights = jnp.concatenate([fresh_weights[None], leave_weights[:-1]], axis=0)
    enter_moment = jnp.concatenate([fresh_momenta[None], leave_moment[:-1]], axis=0)
    final_weights, final_momenta, outputs_second = lax.map(run_segment, (enter_weights, enter_moment, queries[1], key_vectors[1], values[1], token_rates[1]))
    return (jnp.stack([outputs_first, outputs_second]), final_weights, final_momenta)
```

```python
import functools
import jax
import jax.numpy as jnp
from jax import lax
from jax.experimental import pallas as pl
from jax.experimental.pallas import tpu as pltpu
from jax.sharding import PartitionSpec as P

momentum_decay = 0.9
learn_rate = 0.05
epsilon = 1e-06
LANES = 128
MESH = pl.DeviceIdType.MESH
f32 = jnp.float32
bf16 = jnp.bfloat16


def flip(index, mask):
    out, bit = index, 1
    while bit <= mask:
        if mask & bit:
            out = out + bit * (1 - 2 * lax.rem(index // bit, 2))
        bit *= 2
    return out


def pack(matrix):
    width = matrix.shape[1]
    chunks = LANES // width
    high = matrix.shape[0] // chunks
    return jnp.concatenate([matrix[k * high:(k + 1) * high] for k in range(chunks)], axis=1)


def unpack(piece, width):
    chunks = LANES // width
    return jnp.concatenate([piece[:, k * width:(k + 1) * width] for k in range(chunks)], axis=0)


def sigmoid(x):
    return 0.5 + 0.5 * jnp.tanh(0.5 * x)


def mm(a, b):
    return jnp.dot(a, b, preferred_element_type=f32)


def kernel(
    n, segs, steps, blocks, tile,
    k_hbm, v_hbm, q_hbm, rates, w_in, m_in, fw_in, fm_in,
    out_hbm, w_out, m_out,
    kbuf, vbuf, qbuf, obuf, kt, scaled, scaled_t, hid, bgate, bup, wb, wa,
    wstate, mstate, gsend, grecv, own, ent, msend, mrecv, sq,
    load_sem, store_sem, gs_sem, gr_sem, os_sem, or_sem, es_sem, er_sem, ms_sem, mr_sem,
    qs_sem, qr_sem,
):
    total = steps * blocks
    rows, width_all = kbuf.shape[1], kbuf.shape[2]
    width = width_all // n
    chunks = LANES // width
    high = width_all // chunks
    tiles = rows // tile
    seg = lax.axis_index("seg")
    tok = lax.axis_index("tok")
    first = seg == 0
    last = seg == segs - 1
    peers = [flip(tok, d) for d in range(n)]

    def to_peer(d):
        return {"seg": seg, "tok": peers[d]}

    down = {"seg": lax.rem(seg + 1, segs), "tok": tok}
    up = {"seg": lax.rem(seg + segs - 1, segs), "tok": tok}

    def rcopy(src, dst, send, recv, device):
        return pltpu.make_async_remote_copy(
            src_ref=src, dst_ref=dst, send_sem=send, recv_sem=recv,
            device_id=device, device_id_type=MESH,
        )

    loads = [[
        pltpu.make_async_copy(src.at[b], dst.at[b], load_sem.at[j, b])
        for b in range(total)
    ] for j, (src, dst) in enumerate(((k_hbm, kbuf), (v_hbm, vbuf), (q_hbm, qbuf)))]

    barrier = pltpu.get_barrier_semaphore()
    for d in range(1, n):
        pl.semaphore_signal(barrier, inc=1, device_id=to_peer(d), device_id_type=MESH)

    @pl.when(jnp.logical_not(last))
    def _():
        pl.semaphore_signal(barrier, inc=1, device_id=down, device_id_type=MESH)

    @pl.when(jnp.logical_not(first))
    def _():
        pl.semaphore_signal(barrier, inc=1, device_id=up, device_id_type=MESH)

    for b in range(total):
        loads[0][b].start()
        loads[1][b].start()
    for b in range(total):
        loads[2][b].start()

    for m in range(3):
        wstate[m] = pack(w_in[m])
        mstate[m] = pack(m_in[m])
    ent[0, tok] = wstate[...].astype(bf16)
    all_rates = rates[...]
    sums = jnp.sum(all_rates * all_rates, axis=1, keepdims=True)
    sq[tok] = jnp.broadcast_to(sums, (total, LANES))

    @pl.when(first)
    def _():
        for s in range(1, steps):
            for m in range(3):
                ent[s, tok, m] = pack(fw_in[m]).astype(bf16)

    neighbours = (seg + segs - 1) // segs + (2 * segs - 2 - seg) // segs
    pl.semaphore_wait(barrier, n - 1 + neighbours)

    def ent_copy(s, d, device=None):
        return rcopy(
            ent.at[s, tok], ent.at[s, tok], es_sem.at[s, d], er_sem.at[s, d],
            to_peer(d) if device is None else device,
        )

    def sq_copy(d):
        return rcopy(sq.at[tok], sq.at[tok], qs_sem.at[d], qr_sem.at[d], to_peer(d))

    for d in range(1, n):
        ent_copy(0, d).start()
    for d in range(1, n):
        sq_copy(d).start()

    @pl.when(first)
    def _():
        for s in range(1, steps):
            for d in range(1, n):
                ent_copy(s, d).start()

    def g_copy(b, d):
        return rcopy(
            gsend.at[peers[d]], grecv.at[b, d], gs_sem.at[b, d], gr_sem.at[b, d], to_peer(d)
        )

    def own_copy(b, d):
        return rcopy(
            own.at[b, tok], own.at[b, tok], os_sem.at[b, d], or_sem.at[b, d], to_peer(d)
        )

    def relay_copy(b, s, d):
        return rcopy(
            own.at[b, peers[d]], ent.at[s + 1, peers[d]], es_sem.at[s + 1, d],
            er_sem.at[s + 1, d], down,
        )

    def m_copy(s):
        return rcopy(msend.at[s], mrecv.at[s], ms_sem.at[s], mr_sem.at[s], down)

    def restore(source, slot, target):
        for m in range(3):
            for k in range(chunks):
                target[m, k * high:(k + 1) * high, :] = jnp.concatenate(
                    [
                        source[slot, p, m][:, k * width:(k + 1) * width]
                        for p in range(n)
                    ],
                    axis=1,
                )

    def prepare(b):
        pltpu.make_async_copy(k_hbm.at[b], kbuf.at[b], load_sem.at[0, b]).wait()
        pltpu.make_async_copy(v_hbm.at[b], vbuf.at[b], load_sem.at[1, b]).wait()
        kt[...] = kbuf[b].T
        row = jnp.broadcast_to(rates[pl.ds(b, 1), :], (LANES, rows))
        column = jnp.concatenate([row.T] * (width_all // LANES), axis=1)
        product = (column * vbuf[b].astype(f32)).astype(bf16)
        scaled[...] = product
        scaled_t[...] = product.T

    def gradients(b):
        w1, w2, w3 = wb[0], wb[1], wb[2]

        @pl.loop(0, tiles)
        def _(i):
            at = pl.ds(pl.multiple_of(i * tile, tile), tile)
            keys = kbuf[b, at, :]
            gate = mm(keys, w1)
            up_pre = mm(keys, w3)
            back = lax.dot_general(
                scaled[at, :], w2, (((1,), (1,)), ((), ())), preferred_element_type=f32
            )
            sig = sigmoid(gate)
            act = gate * sig
            slope = sig + act * (1.0 - sig)
            hid[at, :] = (act * up_pre).astype(bf16)
            bgate[at, :] = (back * up_pre * slope).astype(bf16)
            bup[at, :] = (back * act).astype(bf16)

        keys_t = kt[...]
        parts = (
            mm(keys_t, bgate[...]),
            mm(scaled_t[...], hid[...]).T,
            mm(keys_t, bup[...]),
        )
        for m in range(3):
            for p in range(n):
                gsend[p, m] = pack(parts[m][:, p * width:(p + 1) * width]).astype(bf16)

    def column_sum(x):
        t = jnp.broadcast_to(jnp.sum(x * x, axis=0, keepdims=True), (8, LANES))
        shift = width
        while shift < LANES:
            t = t + pltpu.roll(t, shift, 1)
            shift *= 2
        return t[:1]

    def update(b):
        square = sq[0, pl.ds(b, 1), :]
        for p in range(1, n):
            square = square + sq[p, pl.ds(b, 1), :]
        factor = lax.rsqrt(square)
        for m in range(3):
            grad = gsend[tok, m].astype(f32)
            for d in range(1, n):
                grad = grad + grecv[b, d, m].astype(f32)
            moment = momentum_decay * mstate[m] - grad * factor
            weight = wstate[m]
            stepped = weight - learn_rate * moment
            rescale = jnp.sqrt(column_sum(weight) / (column_sum(stepped) + epsilon))
            weight = stepped * rescale
            mstate[m] = moment
            wstate[m] = weight
            own[b, tok, m] = weight.astype(bf16)

    def apply_fast(b):
        pltpu.make_async_copy(q_hbm.at[b], qbuf.at[b], load_sem.at[2, b]).wait()
        restore(own, b, wa)
        w1, w2, w3 = wa[0], wa[1], wa[2]

        @pl.loop(0, tiles)
        def _(i):
            at = pl.ds(pl.multiple_of(i * tile, tile), tile)
            asked = qbuf[b, at, :]
            gate = mm(asked, w1)
            hidden = (gate * sigmoid(gate) * mm(asked, w3)).astype(bf16)
            obuf[b, at, :] = mm(hidden, w2).astype(bf16)

        pltpu.make_async_copy(obuf.at[b], out_hbm.at[b], store_sem.at[b]).start()

    prepare(0)
    for d in range(1, n):
        sq_copy(d).wait_recv()

    @pl.loop(0, total)
    def _(b):
        s = b // blocks
        g = b - s * blocks

        @pl.when(g == 0)
        def _():
            for d in range(1, n):
                ent_copy(s, d).wait_recv()

            @pl.when(jnp.logical_and(s > 0, first))
            def _():
                for m in range(3):
                    wstate[m] = pack(fw_in[m])
                    mstate[m] = pack(fm_in[m])

            @pl.when(jnp.logical_and(s > 0, jnp.logical_not(first)))
            def _():
                relay_copy(b - 1, s - 1, 0).wait_recv()
                m_copy(s - 1).wait_recv()
                wstate[...] = ent[s, tok].astype(f32)
                mstate[...] = mrecv[s - 1].astype(f32)

            restore(ent, s, wb)

        @pl.when(g > 0)
        def _():
            restore(own, b - 1, wb)

        gradients(b)
        for d in range(1, n):
            g_copy(b, d).start()

        @pl.when(g > 0)
        def _():
            apply_fast(b - 1)

        for d in range(1, n):
            g_copy(b, d).wait_recv()
        update(b)
        border = jnp.logical_and(g == blocks - 1, s < steps - 1)
        passing = jnp.logical_and(border, jnp.logical_not(last))

        @pl.when(passing)
        def _():
            relay_copy(b, s, 0).start()

        for d in range(1, n):
            own_copy(b, d).start()

        @pl.when(passing)
        def _():
            msend[s] = mstate[...].astype(bf16)
            m_copy(s).start()

        for d in range(1, n):
            g_copy(b, d).wait_send()

        @pl.when(b < total - 1)
        def _():
            prepare(b + 1)

        for d in range(1, n):
            own_copy(b, d).wait_recv()

            @pl.when(passing)
            def _():
                relay_copy(b, s, d).start()

        @pl.when(g == blocks - 1)
        def _():
            apply_fast(b)

        for d in range(1, n):
            own_copy(b, d).wait_send()

        @pl.when(passing)
        def _():
            for d in range(n):
                relay_copy(b, s, d).wait_send()
            m_copy(s).wait_send()

    for m in range(3):
        w_out[m] = unpack(wstate[m], width)
        m_out[m] = unpack(mstate[m], width)

    for d in range(1, n):
        ent_copy(0, d).wait_send()
        sq_copy(d).wait_send()

    @pl.when(first)
    def _():
        for s in range(1, steps):
            for d in range(1, n):
                ent_copy(s, d).wait_send()

    for b in range(total):
        pltpu.make_async_copy(obuf.at[b], out_hbm.at[b], store_sem.at[b]).wait()


def body(n, segs, queries, keys, values, rates, weights, momenta, fresh_w, fresh_m):
    steps, _, blocks, rows, head = queries.shape
    total = steps * blocks
    width = head // n
    high = 2 * width
    tile = 256 if rows % 256 == 0 else rows
    flat = (total, rows, head)
    piece = (3, high, LANES)
    hbm = pl.BlockSpec(memory_space=pl.ANY)
    vmem = pl.BlockSpec(memory_space=pltpu.VMEM)
    dma = pltpu.SemaphoreType.DMA
    big = (rows, head)
    outs = pl.pallas_call(
        functools.partial(kernel, n, segs, steps, blocks, tile),
        out_shape=(
            jax.ShapeDtypeStruct(flat, bf16),
            jax.ShapeDtypeStruct((3, head, width), f32),
            jax.ShapeDtypeStruct((3, head, width), f32),
        ),
        in_specs=[hbm, hbm, hbm, vmem, vmem, vmem, vmem, vmem],
        out_specs=(hbm, vmem, vmem),
        scratch_shapes=[
            pltpu.VMEM(flat, bf16),
            pltpu.VMEM(flat, bf16),
            pltpu.VMEM(flat, bf16),
            pltpu.VMEM(flat, bf16),
            pltpu.VMEM((head, rows), bf16),
            pltpu.VMEM(big, bf16),
            pltpu.VMEM((head, rows), bf16),
            pltpu.VMEM(big, bf16),
            pltpu.VMEM(big, bf16),
            pltpu.VMEM(big, bf16),
            pltpu.VMEM((3, head, head), bf16),
            pltpu.VMEM((3, head, head), bf16),
            pltpu.VMEM(piece, f32),
            pltpu.VMEM(piece, f32),
            pltpu.VMEM((n,) + piece, bf16),
            pltpu.VMEM((total, n) + piece, bf16),
            pltpu.VMEM((total, n) + piece, bf16),
            pltpu.VMEM((steps, n) + piece, bf16),
            pltpu.VMEM((steps,) + piece, bf16),
            pltpu.VMEM((steps,) + piece, bf16),
            pltpu.VMEM((n, total, LANES), f32),
            dma((3, total)),
            dma((total,)),
            dma((total, n)),
            dma((total, n)),
            dma((total, n)),
            dma((total, n)),
            dma((steps, n)),
            dma((steps, n)),
            dma((steps,)),
            dma((steps,)),
            dma((n,)),
            dma((n,)),
        ],
        compiler_params=pltpu.CompilerParams(
            collective_id=0, has_side_effects=True, vmem_limit_bytes=60 * 1024 * 1024
        ),
    )(
        keys.reshape(flat), values.reshape(flat), queries.reshape(flat),
        rates.reshape(total, rows), weights[0], momenta[0], fresh_w, fresh_m,
    )
    return outs[0].reshape(queries.shape), outs[1][None], outs[2][None]


def solution(mesh):
    n, segs = mesh.shape["tok"], mesh.shape["seg"]
    return jax.shard_map(
        functools.partial(body, n, segs),
        mesh=mesh,
        in_specs=(
            P(None, "seg", None, "tok", None),
            P(None, "seg", None, "tok", None),
            P(None, "seg", None, "tok", None),
            P(None, "seg", None, "tok"),
            P("seg", None, None, "tok"),
            P("seg", None, None, "tok"),
            P(None, None, "tok"),
            P(None, None, "tok"),
        ),
        out_specs=(
            P(None, "seg", None, "tok", None),
            P("seg", None, None, "tok"),
            P("seg", None, None, "tok"),
        ),
        check_vma=False,
    )
```

```python
import functools
import jax
import jax.numpy as jnp
from jax import lax
from jax.experimental import pallas as pl
from jax.experimental.pallas import tpu as pltpu
from jax.sharding import PartitionSpec as P

momentum_decay = 0.9
learn_rate = 0.05
epsilon = 1e-06
LANES = 128
UNROLL = 5
MESH = pl.DeviceIdType.MESH
f32 = jnp.float32
bf16 = jnp.bfloat16


def flip(index, mask):
    out, bit = index, 1
    while bit <= mask:
        if mask & bit:
            out = out + bit * (1 - 2 * lax.rem(index // bit, 2))
        bit *= 2
    return out


def sigmoid(x):
    return 0.5 + 0.5 * jnp.tanh(0.5 * x)


def mm(a, b):
    return jnp.dot(a, b, preferred_element_type=f32)


def mm_t(a, b):
    return lax.dot_general(a, b, (((1,), (1,)), ((), ())), preferred_element_type=f32)


def kernel(
    n, segs, steps, blocks, tile,
    k_hbm, v_hbm, q_hbm, rates, w_in, m_in, fw_in, fm_in,
    out_hbm, wstate, mstate,
    kbuf, vbuf, qbuf, obuf, kt, scaled, scaled_t, hid, bgate, bup,
    gsend, grecv, bank, msend, mrecv, sq,
    load_sem, store_sem, gs_sem, gr_sem, os_sem, or_sem, es_sem, er_sem, ms_sem, mr_sem,
    qs_sem, qr_sem,
):
    total = steps * blocks
    rows, head = kbuf.shape[1], kbuf.shape[2]
    width = head // n
    tiles = rows // tile
    order = (1, 0, 2)
    around = tuple(range(n - 1, 0, -1))
    seg = lax.axis_index("seg")
    tok = lax.axis_index("tok")
    first = seg == 0
    last = seg == segs - 1
    peers = [flip(tok, d) for d in range(n)]

    def part(p):
        return pl.ds(pl.multiple_of(p * width, width), width)

    mine = part(tok)

    def to_peer(d):
        return {"seg": seg, "tok": peers[d]}

    down = {"seg": lax.rem(seg + 1, segs), "tok": tok}
    up = {"seg": lax.rem(seg + segs - 1, segs), "tok": tok}

    def rcopy(src, dst, send, recv, device):
        return pltpu.make_async_remote_copy(
            src_ref=src, dst_ref=dst, send_sem=send, recv_sem=recv,
            device_id=device, device_id_type=MESH,
        )

    loads = [[
        pltpu.make_async_copy(src.at[b], dst.at[b], load_sem.at[j, b])
        for b in range(total)
    ] for j, (src, dst) in enumerate(((k_hbm, kbuf), (v_hbm, vbuf), (q_hbm, qbuf)))]

    barrier = pltpu.get_barrier_semaphore()
    for d in range(1, n):
        pl.semaphore_signal(barrier, inc=1, device_id=to_peer(d), device_id_type=MESH)

    @pl.when(jnp.logical_not(last))
    def _():
        pl.semaphore_signal(barrier, inc=1, device_id=down, device_id_type=MESH)

    @pl.when(jnp.logical_not(first))
    def _():
        pl.semaphore_signal(barrier, inc=1, device_id=up, device_id_type=MESH)

    for b in range(total):
        loads[0][b].start()
        loads[1][b].start()
    for b in range(total):
        loads[2][b].start()

    wstate[...] = w_in[...]
    mstate[...] = m_in[...]
    for m in range(3):
        bank[total, m, mine, :] = w_in[m].astype(bf16)
    for s in range(steps):
        drawn = rates[s]
        sums = jnp.sum(drawn * drawn, axis=1, keepdims=True)
        sq[tok, s] = jnp.broadcast_to(sums, (blocks, LANES))

    @pl.when(first)
    def _():
        for s in range(1, steps):
            for m in range(3):
                bank[total + s, m, mine, :] = fw_in[m].astype(bf16)

    neighbours = (seg + segs - 1) // segs + (2 * segs - 2 - seg) // segs
    pl.semaphore_wait(barrier, n - 1 + neighbours)

    def ent_copy(s, d, m):
        place = bank.at[total + s, m, mine, :]
        return rcopy(place, place, es_sem.at[s, d, m], er_sem.at[s, d, m], to_peer(d))

    def sq_copy(d):
        return rcopy(sq.at[tok], sq.at[tok], qs_sem.at[d], qr_sem.at[d], to_peer(d))

    for m in order:
        for d in around:
            ent_copy(0, d, m).start()
    for d in around:
        sq_copy(d).start()

    @pl.when(first)
    def _():
        for s in range(1, steps):
            for m in order:
                for d in around:
                    ent_copy(s, d, m).start()

    def g_copy(b, d, m):
        return rcopy(
            gsend.at[m, part(peers[d]), :], grecv.at[b, d, m],
            gs_sem.at[b, d, m], gr_sem.at[b, d, m], to_peer(d),
        )

    def own_copy(b, d, m):
        place = bank.at[b, m, mine, :]
        return rcopy(place, place, os_sem.at[b, d, m], or_sem.at[b, d, m], to_peer(d))

    def relay_copy(b, s, d, m):
        piece = part(peers[d])
        return rcopy(
            bank.at[b, m, piece, :], bank.at[total + s + 1, m, piece, :],
            es_sem.at[s + 1, d, m], er_sem.at[s + 1, d, m], down,
        )

    def m_copy(s):
        return rcopy(msend.at[s], mrecv.at[s], ms_sem.at[s], mr_sem.at[s], down)

    def prepare(b):
        pltpu.make_async_copy(k_hbm.at[b], kbuf.at[b], load_sem.at[0, b]).wait()
        pltpu.make_async_copy(v_hbm.at[b], vbuf.at[b], load_sem.at[1, b]).wait()
        kt[...] = kbuf[b].T
        s = b // blocks
        row = jnp.broadcast_to(rates[s, pl.ds(b - s * blocks, 1), :], (LANES, rows))
        column = jnp.concatenate([row.T] * (head // LANES), axis=1)
        product = (column * vbuf[b].astype(f32)).astype(bf16)
        scaled[...] = product
        scaled_t[...] = product.T

    def gradients(b, slot):
        w1, w2, w3 = bank[slot, 0], bank[slot, 1], bank[slot, 2]

        @pl.loop(0, tiles, unroll=UNROLL)
        def _(i):
            at = pl.ds(pl.multiple_of(i * tile, tile), tile)
            keys = kbuf[b, at, :]
            back = mm(scaled[at, :], w2)
            gate = mm_t(keys, w1)
            up_pre = mm_t(keys, w3)
            sig = sigmoid(gate)
            act = gate * sig
            slope = sig + act * (1.0 - sig)
            hid[at, :] = (act * up_pre).astype(bf16)
            bgate[at, :] = (back * up_pre * slope).astype(bf16)
            bup[at, :] = (back * act).astype(bf16)

        for m in order:
            if m == 1:
                grad = mm(scaled_t[...], hid[...])
            else:
                grad = mm(kt[...], (bgate if m == 0 else bup)[...]).T
            gsend[m] = grad.astype(bf16)
            for d in around:
                g_copy(b, d, m).start()

    def update(b, m, factor):
        grad = gsend[m, mine, :].astype(f32)
        for d in range(1, n):
            grad = grad + grecv[b, d, m].astype(f32)
        moment = momentum_decay * mstate[m] - grad * factor
        weight = wstate[m]
        stepped = weight - learn_rate * moment
        before = jnp.sum(weight * weight, axis=1, keepdims=True)
        after = jnp.sum(stepped * stepped, axis=1, keepdims=True)
        weight = stepped * jnp.sqrt(before / (after + epsilon))
        mstate[m] = moment
        wstate[m] = weight
        bank[b, m, mine, :] = weight.astype(bf16)

    def apply_fast(b):
        pltpu.make_async_copy(q_hbm.at[b], qbuf.at[b], load_sem.at[2, b]).wait()
        w1, w2, w3 = bank[b, 0], bank[b, 1], bank[b, 2]

        @pl.loop(0, tiles, unroll=UNROLL)
        def _(i):
            at = pl.ds(pl.multiple_of(i * tile, tile), tile)
            asked = qbuf[b, at, :]
            gate = mm_t(asked, w1)
            hidden = (gate * sigmoid(gate) * mm_t(asked, w3)).astype(bf16)
            obuf[b, at, :] = mm_t(hidden, w2).astype(bf16)

        pltpu.make_async_copy(obuf.at[b], out_hbm.at[b], store_sem.at[b]).start()

    prepare(0)
    for d in range(1, n):
        sq_copy(d).wait_recv()

    @pl.loop(0, total)
    def _(b):
        s = b // blocks
        g = b - s * blocks
        inner = (g + blocks - 1) // blocks
        entered = jnp.logical_and(jnp.logical_and(g == 0, s > 0), jnp.logical_not(first))

        @pl.when(g == 0)
        def _():
            for m in order:
                for d in around:
                    ent_copy(s, d, m).wait_recv()

        @pl.when(jnp.logical_and(jnp.logical_and(g == 0, s > 0), first))
        def _():
            wstate[...] = fw_in[...]
            mstate[...] = fm_in[...]

        @pl.when(entered)
        def _():
            for m in order:
                relay_copy(b - 1, s - 1, 0, m).wait_recv()
                wstate[m] = bank[total + s, m, mine, :].astype(f32)

        gradients(b, (total + s) * (1 - inner) + (b - 1) * inner)

        @pl.when(g > 0)
        def _():
            apply_fast(b - 1)

        @pl.when(entered)
        def _():
            m_copy(s - 1).wait_recv()
            mstate[...] = mrecv[s - 1].astype(f32)

        border = jnp.logical_and(g == blocks - 1, s < steps - 1)
        passing = jnp.logical_and(border, jnp.logical_not(last))
        square = sq[0, s, pl.ds(g, 1), :]
        for p in range(1, n):
            square = square + sq[p, s, pl.ds(g, 1), :]
        factor = lax.rsqrt(jnp.concatenate([square] * (head // LANES), axis=1))

        for m in order:
            for d in around:
                g_copy(b, d, m).wait_recv()
            update(b, m, factor)

            @pl.when(passing)
            def _():
                relay_copy(b, s, 0, m).start()

            for d in around:
                own_copy(b, d, m).start()

        @pl.when(passing)
        def _():
            msend[s] = mstate[...].astype(bf16)
            m_copy(s).start()

        for m in order:
            for d in around:
                g_copy(b, d, m).wait_send()

        @pl.when(b < total - 1)
        def _():
            prepare(b + 1)

        for m in order:
            for d in range(1, n):
                own_copy(b, d, m).wait_recv()

                @pl.when(passing)
                def _():
                    relay_copy(b, s, d, m).start()

        @pl.when(g == blocks - 1)
        def _():
            apply_fast(b)

        for m in order:
            for d in around:
                own_copy(b, d, m).wait_send()

        @pl.when(passing)
        def _():
            for m in order:
                for d in range(n):
                    relay_copy(b, s, d, m).wait_send()
            m_copy(s).wait_send()

    for d in around:
        sq_copy(d).wait_send()
        for m in order:
            ent_copy(0, d, m).wait_send()

    @pl.when(first)
    def _():
        for s in range(1, steps):
            for m in order:
                for d in around:
                    ent_copy(s, d, m).wait_send()

    for b in range(total):
        pltpu.make_async_copy(obuf.at[b], out_hbm.at[b], store_sem.at[b]).wait()


def body(n, segs, queries, keys, values, rates, weights, momenta, fresh_w, fresh_m):
    steps, _, blocks, rows, head = queries.shape
    total = steps * blocks
    width = head // n
    tile = 256 if rows % 256 == 0 else rows
    flat = (total, rows, head)
    piece = (3, width, head)
    hbm = pl.BlockSpec(memory_space=pl.ANY)
    vmem = pl.BlockSpec(memory_space=pltpu.VMEM)
    dma = pltpu.SemaphoreType.DMA
    big = (rows, head)
    turned = (head, rows)
    outs = pl.pallas_call(
        functools.partial(kernel, n, segs, steps, blocks, tile),
        out_shape=(
            jax.ShapeDtypeStruct(flat, bf16),
            jax.ShapeDtypeStruct(piece, f32),
            jax.ShapeDtypeStruct(piece, f32),
        ),
        in_specs=[hbm, hbm, hbm, vmem, vmem, vmem, vmem, vmem],
        out_specs=(hbm, vmem, vmem),
        scratch_shapes=[pltpu.VMEM(flat, bf16)] * 4
        + [
            pltpu.VMEM(turned, bf16),
            pltpu.VMEM(big, bf16),
            pltpu.VMEM(turned, bf16),
            pltpu.VMEM(big, bf16),
            pltpu.VMEM(big, bf16),
            pltpu.VMEM(big, bf16),
            pltpu.VMEM((3, head, head), bf16),
            pltpu.VMEM((total, n) + piece, bf16),
            pltpu.VMEM((total + steps, 3, head, head), bf16),
            pltpu.VMEM((steps,) + piece, bf16),
            pltpu.VMEM((steps,) + piece, bf16),
            pltpu.VMEM((n, steps, blocks, LANES), f32),
            dma((3, total)),
            dma((total,)),
            dma((total, n, 3)),
            dma((total, n, 3)),
            dma((total, n, 3)),
            dma((total, n, 3)),
            dma((steps, n, 3)),
            dma((steps, n, 3)),
            dma((steps,)),
            dma((steps,)),
            dma((n,)),
            dma((n,)),
        ],
        compiler_params=pltpu.CompilerParams(
            collective_id=0, has_side_effects=True, vmem_limit_bytes=60 * 1024 * 1024
        ),
    )(
        keys.reshape(flat), values.reshape(flat), queries.reshape(flat), rates[:, 0],
        jnp.swapaxes(weights[0], 1, 2), jnp.swapaxes(momenta[0], 1, 2),
        jnp.swapaxes(fresh_w, 1, 2), jnp.swapaxes(fresh_m, 1, 2),
    )
    return (
        outs[0].reshape(queries.shape),
        jnp.swapaxes(outs[1], 1, 2)[None],
        jnp.swapaxes(outs[2], 1, 2)[None],
    )


def solution(mesh):
    n, segs = mesh.shape["tok"], mesh.shape["seg"]
    return jax.shard_map(
        functools.partial(body, n, segs),
        mesh=mesh,
        in_specs=(
            P(None, "seg", None, "tok", None),
            P(None, "seg", None, "tok", None),
            P(None, "seg", None, "tok", None),
            P(None, "seg", None, "tok"),
            P("seg", None, None, "tok"),
            P("seg", None, None, "tok"),
            P(None, None, "tok"),
            P(None, None, "tok"),
        ),
        out_specs=(
            P(None, "seg", None, "tok", None),
            P("seg", None, None, "tok"),
            P("seg", None, None, "tok"),
        ),
        check_vma=False,
    )
```
